32 devices in a mesh: pairs: 8 (over y, x, core), aux: 4 (over z).
Axes of the slice: x: 2, y: 2, z: 4, core: 2. Of those that a mesh axis runs over, the one named last changes fastest.
Arguments:
- factors: bfloat16 [4096, 128, 128], P('aux', 'pairs'), may hold values from -1 to 1
- coefficients: bfloat16 [128, 256, 128], P(('pairs', 'aux')), may hold values from -0.375 to 0.375
- amplitudes: bfloat16 [128, 128, 128], P(('pairs', 'aux')), may hold values from -6 to 6
- domains: int32 [128, 256], P(('pairs', 'aux')), may hold values from 0 to 573, as said below
- partners: int32 [128, 12], P(('pairs', 'aux')), may hold values from 0 to 127, as said below
- couplings: float32 [128, 12], P(('pairs', 'aux')), may hold values from -4 to 4
- energies: float32 [128, 128], P(('pairs', 'aux')), may hold values from 0.5 to 4
Outputs:
- residual: float32 [128, 128, 128], P(('pairs', 'aux'))
The draws below stay inside these ranges and needn't reach their ends.
Inputs may be any that keep to these rules, and one draw needn't show every extreme that they name: `partners`: row p names 12 different pairs other than p, all within the run of 17 consecutive pair numbers centred on p, moved inward where it would pass 0 or 127. `domains`: each row holds 256 different function numbers.
All inputs are finite; a program needn't handle non-finite values.
Results may differ from the reference program's by a relative error of at most 0.0065.
Values may be sent and summed in bfloat16 or wider, within the bound.
No kernel may reach another device: no remote copies, remote signals or barrier semaphores. Data moves between devices by JAX's collectives and lax.ppermute only.
A program may use at most 128 MiB of HBM per device.

```python
import math
import jax
import jax.numpy as jnp
from jax import lax

NCPL = 12
NPNO = 128
DOM = 256
NAUX = 4096
PAIRS = 128
SPAN = 8
AUX_SLAB = 1024
N_AUX = 4


def draw_partners(key, part):
    reach_pairs = SPAN
    pair_ids = jnp.arange(PAIRS, dtype=jnp.int32)
    starts = jnp.clip(pair_ids - reach_pairs, 0, PAIRS - 1 - 2 * reach_pairs)
    offsets = jnp.arange(2 * reach_pairs + 1, dtype=jnp.int32)
    scores = jax.random.randint(jax.random.fold_in(key, 11), (PAIRS, 2 * reach_pairs + 1), 0, 1 << 20, dtype=jnp.int32)
    scores = scores * 1024 + offsets[None, :]
    scores = jnp.where(offsets[None, :] == (pair_ids - starts)[:, None], 2147483647, scores)
    order = jnp.argsort(scores, axis=1, stable=True).astype(jnp.int32)
    return (starts[:, None] + order[:, :NCPL]).astype(jnp.int32)


def draw_domains(key, part):
    step_size = DOM // 128
    window_len = DOM + DOM // 4
    pair_ids = jnp.arange(PAIRS, dtype=jnp.int32)
    starts = pair_ids * step_size
    offsets = jnp.arange(window_len, dtype=jnp.int32)
    scores = jax.random.randint(jax.random.fold_in(key, 23), (PAIRS, window_len), 0, 1 << 20, dtype=jnp.int32)
    scores = scores * 1024 + offsets[None, :]
    order = jnp.argsort(scores, axis=1, stable=True).astype(jnp.int32)
    return (starts[:, None] + order[:, :DOM]).astype(jnp.int32)


def draw_factors(key, part):
    slab_count = NAUX // AUX_SLAB
    identity = jnp.eye(NPNO, dtype=jnp.float32)
    total_scale = 8.0
    level_reach = 1.1
    mean_power = (math.exp(2.0 * level_reach) - math.exp(-2.0 * level_reach)) / (4.0 * level_reach)
    row_scale = math.sqrt(total_scale / (NAUX * mean_power))

    def one_pair(pair_id):
        pair_key = jax.random.fold_in(jax.random.fold_in(key, 31), pair_id)
        noise_key = jax.random.fold_in(pair_key, 1)
        mix_key = jax.random.fold_in(pair_key, 2)
        level_key = jax.random.fold_in(pair_key, 3)
        own_mix = jax.random.normal(mix_key, (NPNO, NPNO), jnp.float32)
        noise = jnp.clip(jax.random.normal(noise_key, (NAUX, NPNO), jnp.float32), -5.0, 5.0)
        mixing = identity + own_mix / math.sqrt(NPNO)
        levels = jax.random.uniform(level_key, (slab_count,), jnp.float32, -level_reach, level_reach)
        slab_weights = jnp.repeat(jnp.exp(levels), AUX_SLAB)
        rows = jnp.dot(noise, mixing, precision=lax.Precision.HIGHEST)
        rows = rows * (slab_weights * row_scale)[:, None]
        return jnp.clip(rows, -1.0, 1.0).astype(jnp.bfloat16)
    stacked = lax.map(one_pair, jnp.arange(PAIRS, dtype=jnp.int32))
    return jnp.transpose(stacked, (1, 0, 2))


def shard_levels(stream_key, extent, shards, least, top_value):
    def one(axis_at, parts):
        heights = jax.random.uniform(jax.random.fold_in(jax.random.fold_in(stream_key, 6), axis_at), (parts,), jnp.float32, least / len(shards), top_value / len(shards))
        return jnp.repeat(jnp.exp(heights), extent[axis_at] // parts).reshape((-1,) + (1,) * (len(extent) - axis_at - 1))

    gain = one(*shards[0])
    for cut in shards[1:]:
        gain = gain * one(*cut)
    return gain


def bell_draw(own_key, extent, deviation, most, cuts=(), kind=jnp.bfloat16):
    result = jax.random.normal(own_key, extent, jnp.float32) * deviation
    if len(cuts) > 0:
        result = shard_levels(own_key, extent, cuts, -0.22, 0.18) * result
    return jnp.clip(result, min=-most, max=most).astype(kind)


def setup_inputs(seed: int = 0) -> dict:
    splits = jax.random.split(jax.random.key(seed), 8)
    factors = draw_factors(jax.random.fold_in(splits[7], 71), 0)
    coefficients = bell_draw(splits[1], (PAIRS, DOM, NPNO), DOM ** -0.5, 0.375, ((0, 32),))
    amplitudes = bell_draw(splits[2], (PAIRS, NPNO, NPNO), 1.0, 6.0, ((0, 32),))
    domains = draw_domains(jax.random.fold_in(splits[7], 71), 0)
    partners = draw_partners(jax.random.fold_in(splits[7], 71), 0)
    couplings = bell_draw(splits[5], (PAIRS, NCPL), 1.0, 4.0, ((0, 32),), jnp.float32)
    energies = jnp.clip(jnp.exp(math.log(4.0) - 2.0794415 * jax.random.uniform(splits[6], (PAIRS, NPNO), jnp.float32) ** shard_levels(splits[6], (PAIRS, NPNO), ((0, 32),), -0.2, 0.2)), 0.5, 4.0)
    return {"factors": factors, "coefficients": coefficients, "amplitudes": amplitudes, "domains": domains, "partners": partners, "couplings": couplings, "energies": energies}


def reference(factors, coefficients, amplitudes, domains, partners, couplings, energies):
    def per_pair(pair_id):
        aux_column = lax.dynamic_index_in_dim(factors, pair_id, 1, keepdims=False)
        slab_rows = aux_column.astype(jnp.float32).reshape(N_AUX, NAUX // N_AUX, NPNO)
        slab_terms = jnp.einsum("sxa,sxb->sab", slab_rows, slab_rows, precision=lax.Precision.HIGHEST)
        slab_terms = lax.optimization_barrier(slab_terms.astype(jnp.bfloat16)).astype(jnp.float32)
        exchange_k = jnp.sum(slab_terms, axis=0)
        listed = partners[pair_id]
        own_coeff = coefficients[pair_id]
        own_funcs = domains[pair_id]
        far_coeff = coefficients[listed]
        far_amps = amplitudes[listed]
        far_funcs = domains[listed]
        same_func = own_funcs[None, :, None] == far_funcs[:, None, :]
        has_match = jnp.any(same_func, axis=2)
        position = jnp.sum(jnp.where(same_func, jnp.arange(DOM, dtype=jnp.int32)[None, None, :], 0), axis=2, dtype=jnp.int32).astype(jnp.int32)
        picked = jax.vmap(lambda rows, where_rows: rows[where_rows])(far_coeff, position)
        matched = jnp.where(has_match[:, :, None], picked, jnp.zeros((), jnp.bfloat16))
        intersection = jnp.einsum("fa,cfn->can", own_coeff.astype(jnp.float32), matched.astype(jnp.float32), precision=lax.Precision.HIGHEST).astype(jnp.bfloat16)
        mixed_rows = jnp.einsum("can,cnm->cam", intersection.astype(jnp.float32), far_amps.astype(jnp.float32), precision=lax.Precision.HIGHEST).astype(jnp.bfloat16)
        coupled = jnp.einsum("cam,cbm->cab", mixed_rows.astype(jnp.float32), intersection.astype(jnp.float32), precision=lax.Precision.HIGHEST)
        cycle_term = jnp.sum(couplings[pair_id][:, None, None] * coupled, axis=0)
        pair_energy = energies[pair_id]
        diagonal_term = (pair_energy[:, None] + pair_energy[None, :]) * amplitudes[pair_id].astype(jnp.float32)
        return exchange_k + diagonal_term - cycle_term

    return lax.map(per_pair, jnp.arange(PAIRS, dtype=jnp.int32))
```

```python
import functools

import jax
import jax.numpy as jnp
from jax import lax
from jax.experimental import pallas as pl
from jax.experimental.pallas import tpu as pltpu
from jax.sharding import PartitionSpec as P

BF16 = jnp.bfloat16
F32 = jnp.float32
WHOLE = pl.BlockSpec(memory_space=pltpu.VMEM)


def meta_rows(dom_width, lanes, weight_count):
    rows = 2 * (dom_width // lanes) + 2 * -(-weight_count // lanes)
    return -(-rows // 16) * 16


def pack_body(ids, coeff, amps, dom, partners, couplings, sent, hosted, *, aux_count):
    own, width, lanes = coeff.shape
    slots = 2 * own
    group = own * aux_count
    weight_rows = -(-aux_count * slots // lanes)
    at = lax.broadcasted_iota(jnp.int32, (1, weight_rows * lanes), 1)
    host, slot = at // slots, at % slots
    first = ids[0] + host * own
    beside = jnp.where(host < aux_count // 2, group, -group)
    number = jnp.where(slot < own, first + slot, first + slot - own + beside)
    number = jnp.where(host < aux_count, number, -1)
    listed, strength = partners[...], couplings[...]
    weight = jnp.zeros((own, weight_rows * lanes), F32)
    for c in range(listed.shape[1]):
        weight += jnp.where(listed[:, c : c + 1] == number, strength[:, c : c + 1], 0.0)
    coarse = weight.astype(BF16).astype(F32)
    fine = weight - coarse
    funcs = dom[...]
    high = (funcs >> 8).astype(F32)
    low = (funcs & 255).astype(F32)
    extra = meta_rows(width, lanes, aux_count * slots)
    for p in range(own):
        rows = []
        for part in (high, low, coarse, fine):
            for k in range(part.shape[1] // lanes):
                rows.append(part[p : p + 1, k * lanes : (k + 1) * lanes])
        rows.append(jnp.zeros((extra - len(rows), lanes), F32))
        meta = jnp.concatenate(rows, axis=0).astype(BF16)
        orbitals = coeff[p]
        sent[p, :width] = orbitals
        sent[p, width:] = meta
        hosted[p, :width] = orbitals
        hosted[p, width : width + extra] = meta
        hosted[p, width + extra :] = amps[p]


def functions_of(meta, width, lanes):
    parts = width // lanes
    return [meta[k : k + 1] * 256.0 + meta[parts + k : parts + k + 1] for k in range(parts)]


def terms_body(ids, sent, near, beside, exchange, out, *, width):
    own, _, lanes = sent.shape
    extra = sent.shape[1] - width
    slots = 2 * own
    parts = width // lanes
    place = ids[0] * slots
    sources = [(near, j) for j in range(own)] + [(beside, j) for j in range(own)]
    far_funcs = []
    for ref, j in sources:
        meta = ref[j, width : width + extra].astype(F32)
        far_funcs.append(jnp.concatenate(functions_of(meta, width, lanes), axis=1))
    for p in range(own):
        meta = sent[p, width:].astype(F32)
        funcs = jnp.concatenate(functions_of(meta, width, lanes), axis=1)
        column = jnp.transpose(jnp.broadcast_to(funcs, (8, width)))[:, :1]
        weights = meta[2 * parts : 2 * parts + 1] + meta[2 * parts + 1 : 2 * parts + 2]
        lane = lax.broadcasted_iota(jnp.int32, (1, lanes), 1)
        matched = []
        for (ref, j), row in zip(sources, far_funcs):
            same = jnp.where(column == row, 1.0, 0.0).astype(BF16)
            matched.append(
                jnp.dot(same, ref[j, :width], preferred_element_type=F32).astype(BF16)
            )
        overlap = lax.dot_general(
            sent[p, :width],
            jnp.concatenate(matched, axis=1),
            (((0,), (0,)), ((), ())),
            preferred_element_type=F32,
        ).astype(BF16)
        mixed = []
        for k, (ref, j) in enumerate(sources):
            weight = jnp.sum(jnp.where(lane == place + k, weights, 0.0), axis=1, keepdims=True)
            part = jnp.dot(
                overlap[:, k * lanes : (k + 1) * lanes],
                ref[j, width + extra :],
                preferred_element_type=F32,
            )
            mixed.append((part * weight).astype(BF16))
        coupled = lax.dot_general(
            jnp.concatenate(mixed, axis=1),
            overlap,
            (((1,), (1,)), ((), ())),
            preferred_element_type=F32,
        )
        out[p] = (exchange[p] - coupled).astype(out.dtype)


def shards(factors, coefficients, amplitudes, domains, partners, couplings, energies):
    own, width, lanes = coefficients.shape
    aux_count = lax.axis_size("aux")
    group_count = lax.axis_size("pairs")
    half = aux_count // 2
    extra = meta_rows(width, lanes, aux_count * 2 * own)
    group_at = lax.axis_index("pairs")
    aux_at = lax.axis_index("aux")
    smem = pl.BlockSpec(memory_space=pltpu.SMEM)

    sent, hosted = pl.pallas_call(
        functools.partial(pack_body, aux_count=aux_count),
        out_shape=(
            jax.ShapeDtypeStruct((own, width + extra, lanes), BF16),
            jax.ShapeDtypeStruct((own, width + extra + lanes, lanes), BF16),
        ),
        in_specs=[smem, WHOLE, WHOLE, WHOLE, WHOLE, WHOLE],
        out_specs=(WHOLE, WHOLE),
        name="pack",
    )(
        (group_at * own * aux_count).reshape(1).astype(jnp.int32),
        coefficients, amplitudes, domains, partners, couplings,
    )

    routes = []
    for g in range(group_count):
        for z in range(aux_count):
            to = g - 1 if z < half else g + 1
            if 0 <= to < group_count:
                routes.append((g * aux_count + z, to * aux_count + z))
    beside = lax.ppermute(hosted, ("pairs", "aux"), routes)
    order = sorted(range(1, aux_count), key=lambda s: -min(s, aux_count - s))
    arrived = {0: sent}
    for s in order:
        arrived[s] = lax.ppermute(sent, "aux", [((i + s) % aux_count, i) for i in range(aux_count)])

    exchange = jnp.einsum("xpa,xpb->pab", factors, factors, preferred_element_type=F32)

    def terms(s, dtype):
        ids = jnp.stack([aux_at, (aux_at + s) % aux_count]).astype(jnp.int32)
        whole = lambda a: pl.BlockSpec(a.shape, lambda i, ids: (0,) * a.ndim)
        return pl.pallas_call(
            functools.partial(terms_body, width=width),
            grid_spec=pltpu.PrefetchScalarGridSpec(
                num_scalar_prefetch=1,
                grid=(1,),
                in_specs=[
                    whole(arrived[s]), whole(hosted), whole(beside),
                    pl.BlockSpec((own, lanes, lanes), lambda i, ids: (ids[1], 0, 0)),
                ],
                out_specs=pl.BlockSpec((own, lanes, lanes), lambda i, ids: (0, 0, 0)),
            ),
            out_shape=jax.ShapeDtypeStruct((own, lanes, lanes), dtype),
            name="terms",
        )(ids, arrived[s], hosted, beside, exchange)

    returned = [
        lax.ppermute(terms(s, BF16), "aux", [(i, (i + s) % aux_count) for i in range(aux_count)])
        for s in order
    ]
    total = terms(0, F32)
    total += (energies[:, :, None] + energies[:, None, :]) * amplitudes.astype(F32)
    for part in returned:
        total += part.astype(F32)
    return total


def solution(mesh):
    return jax.shard_map(
        shards,
        mesh=mesh,
        in_specs=(
            P("aux", "pairs", None),
            P(("pairs", "aux"), None, None),
            P(("pairs", "aux"), None, None),
            P(("pairs", "aux"), None),
            P(("pairs", "aux"), None),
            P(("pairs", "aux"), None),
            P(("pairs", "aux"), None),
        ),
        out_specs=P(("pairs", "aux"), None, None),
        check_vma=False,
    )
```

```python
import functools

import jax
import jax.numpy as jnp
from jax import lax
from jax.experimental import pallas as pl
from jax.experimental.pallas import tpu as pltpu
from jax.sharding import PartitionSpec as P

BF16 = jnp.bfloat16
F32 = jnp.float32
GRANT = 16 << 20
WHOLE = pl.BlockSpec(memory_space=pltpu.VMEM)
SMEM = pl.BlockSpec(memory_space=pltpu.SMEM)
FAR = pl.BlockSpec(memory_space=pltpu.HBM)


def kept(array):
    return pltpu.with_memory_space_constraint(array, pltpu.VMEM)


def meta_rows(dom_width, lanes, weight_count):
    rows = 2 * (dom_width // lanes) + 2 * -(-weight_count // lanes)
    return -(-rows // 16) * 16


def pack_body(ids, coeff, amps, dom, partners, couplings, sent, hosted, funcs_at, listed_at, strength_at, sems, *, aux_count):
    own, width, lanes = coeff.shape
    slots = 2 * own
    extra = meta_rows(width, lanes, aux_count * slots)
    moves = [
        (listed_at, partners), (strength_at, couplings), (funcs_at, dom),
        (sent.at[:, :width], coeff), (hosted.at[:, :width], coeff), (hosted.at[:, width + extra :], amps),
    ]
    copies = [pltpu.make_async_copy(src, dst, sems.at[k]) for k, (dst, src) in enumerate(moves)]
    for copy in copies:
        copy.start()
    for copy in copies[:3]:
        copy.wait()
    group = own * aux_count
    weight_rows = -(-aux_count * slots // lanes)
    at = lax.broadcasted_iota(jnp.int32, (1, weight_rows * lanes), 1)
    host, slot = at // slots, at % slots
    first = ids[0] + host * own
    beside = jnp.where(host < aux_count // 2, group, -group)
    number = jnp.where(slot < own, first + slot, first + slot - own + beside)
    number = jnp.where(host < aux_count, number, -1)
    listed, strength = listed_at[...], strength_at[...]
    weight = jnp.zeros((own, weight_rows * lanes), F32)
    for c in range(listed.shape[1]):
        weight += jnp.where(listed[:, c : c + 1] == number, strength[:, c : c + 1], 0.0)
    coarse = weight.astype(BF16).astype(F32)
    fine = weight - coarse
    funcs = funcs_at[...]
    high = (funcs >> 8).astype(F32)
    low = (funcs & 255).astype(F32)
    for p in range(own):
        rows = []
        for part in (high, low, coarse, fine):
            for k in range(part.shape[1] // lanes):
                rows.append(part[p : p + 1, k * lanes : (k + 1) * lanes])
        rows.append(jnp.zeros((extra - len(rows), lanes), F32))
        meta = jnp.concatenate(rows, axis=0).astype(BF16)
        sent[p, width:] = meta
        hosted[p, width : width + extra] = meta
    for copy in copies[3:]:
        copy.wait()


def functions_of(meta, width, lanes):
    parts = width // lanes
    return [meta[k : k + 1] * 256.0 + meta[parts + k : parts + k + 1] for k in range(parts)]


def terms_body(ids, sent, near, beside, exchange, out, *, width, shift, aux_count):
    own, _, lanes = sent.shape
    target = lax.rem(ids[0] + shift, aux_count) * own
    extra = sent.shape[1] - width
    slots = 2 * own
    parts = width // lanes
    place = ids[0] * slots
    sources = [(near, j) for j in range(own)] + [(beside, j) for j in range(own)]
    far_funcs = []
    for ref, j in sources:
        meta = ref[j, width : width + extra].astype(F32)
        far_funcs.append(jnp.concatenate(functions_of(meta, width, lanes), axis=1))
    for p in range(own):
        meta = sent[p, width:].astype(F32)
        funcs = jnp.concatenate(functions_of(meta, width, lanes), axis=1)
        column = jnp.transpose(jnp.broadcast_to(funcs, (8, width)))[:, :1]
        weights = meta[2 * parts : 2 * parts + 1] + meta[2 * parts + 1 : 2 * parts + 2]
        lane = lax.broadcasted_iota(jnp.int32, (1, lanes), 1)
        matched = []
        for (ref, j), row in zip(sources, far_funcs):
            same = jnp.where(column == row, 1.0, 0.0).astype(BF16)
            matched.append(
                jnp.dot(same, ref[j, :width], preferred_element_type=F32).astype(BF16)
            )
        overlap = lax.dot_general(
            sent[p, :width],
            jnp.concatenate(matched, axis=1),
            (((0,), (0,)), ((), ())),
            preferred_element_type=F32,
        ).astype(BF16)
        mixed = []
        for k, (ref, j) in enumerate(sources):
            weight = jnp.sum(jnp.where(lane == place + k, weights, 0.0), axis=1, keepdims=True)
            part = jnp.dot(
                overlap[:, k * lanes : (k + 1) * lanes],
                ref[j, width + extra :],
                preferred_element_type=F32,
            )
            mixed.append((part * weight).astype(BF16))
        coupled = lax.dot_general(
            jnp.concatenate(mixed, axis=1),
            overlap,
            (((1,), (1,)), ((), ())),
            preferred_element_type=F32,
        )
        out[p] = (exchange[target + p] - coupled).astype(out.dtype)


def shards(factors, coefficients, amplitudes, domains, partners, couplings, energies):
    own, width, lanes = coefficients.shape
    aux_count = lax.axis_size("aux")
    group_count = lax.axis_size("pairs")
    half = aux_count // 2
    extra = meta_rows(width, lanes, aux_count * 2 * own)
    group_at = lax.axis_index("pairs")
    aux_at = lax.axis_index("aux")

    sent, hosted = pl.pallas_call(
        functools.partial(pack_body, aux_count=aux_count),
        out_shape=(
            pltpu.VMEM((own, width + extra, lanes), BF16),
            pltpu.VMEM((own, width + extra + lanes, lanes), BF16),
        ),
        in_specs=[SMEM, FAR, FAR, FAR, FAR, FAR],
        out_specs=(WHOLE, WHOLE),
        scratch_shapes=[
            pltpu.VMEM(domains.shape, domains.dtype),
            pltpu.VMEM(partners.shape, partners.dtype),
            pltpu.VMEM(couplings.shape, couplings.dtype),
            pltpu.SemaphoreType.DMA((6,)),
        ],
        compiler_params=pltpu.CompilerParams(vmem_limit_bytes=GRANT),
        name="pack",
    )(
        (group_at * own * aux_count).reshape(1).astype(jnp.int32),
        *(
            pltpu.with_memory_space_constraint(a, pltpu.HBM)
            for a in (coefficients, amplitudes, domains, partners, couplings)
        ),
    )

    routes = []
    for g in range(group_count):
        for z in range(aux_count):
            to = g - 1 if z < half else g + 1
            if 0 <= to < group_count:
                routes.append((g * aux_count + z, to * aux_count + z))
    beside = lax.ppermute(hosted, ("pairs", "aux"), routes)
    order = sorted(range(1, aux_count), key=lambda s: -min(s, aux_count - s))
    arrived = {0: sent}
    for s in order:
        arrived[s] = lax.ppermute(sent, "aux", [((i + s) % aux_count, i) for i in range(aux_count)])

    exchange = jnp.einsum("xpa,xpb->pab", factors, factors, preferred_element_type=F32)

    exchange, beside = kept(exchange), kept(beside)
    place = aux_at.reshape(1).astype(jnp.int32)

    def terms(s, dtype):
        return pl.pallas_call(
            functools.partial(terms_body, width=width, shift=s, aux_count=aux_count),
            in_specs=[SMEM, WHOLE, WHOLE, WHOLE, WHOLE],
            out_specs=WHOLE,
            out_shape=pltpu.VMEM((own, lanes, lanes), dtype),
            compiler_params=pltpu.CompilerParams(vmem_limit_bytes=GRANT),
            name="terms",
        )(place, kept(arrived[s]), kept(hosted), beside, exchange)

    returned = [
        lax.ppermute(terms(s, BF16), "aux", [(i, (i + s) % aux_count) for i in range(aux_count)])
        for s in order
    ]
    total = terms(0, F32)
    total += (energies[:, :, None] + energies[:, None, :]) * amplitudes.astype(F32)
    for part in returned:
        total += part.astype(F32)
    return total


def solution(mesh):
    return jax.shard_map(
        shards,
        mesh=mesh,
        in_specs=(
            P("aux", "pairs", None),
            P(("pairs", "aux"), None, None),
            P(("pairs", "aux"), None, None),
            P(("pairs", "aux"), None),
            P(("pairs", "aux"), None),
            P(("pairs", "aux"), None),
            P(("pairs", "aux"), None),
        ),
        out_specs=P(("pairs", "aux"), None, None),
        check_vma=False,
    )
```
